32 devices in a mesh: emb: 8 (over z, core), dp: 4 (over y, x).
Axes of the slice: x: 2, y: 2, z: 4, core: 2. Of those that a mesh axis runs over, the one named last changes fastest.
Arguments:
- embeddings: bfloat16 [512, 256, 256], P('emb', 'dp'), may hold values from -9 to 9
- machine_projection: bfloat16 [512, 32], replicated, may hold values from -0.015625 to 0.015625
- w_lcb: bfloat16 [512, 512], P('dp'), may hold values from -0.25 to 0.25
- w_fmb: bfloat16 [32, 256], replicated, may hold values from -1 to 1
- ln_gain: float32 [512, 256], P('emb'), may hold values from 0.5 to 1.5
- ln_bias: float32 [512, 256], P('emb'), may hold values from -1.8 to 1.8
Outputs:
- layer_out: bfloat16 [512, 256, 256], P('emb', 'dp')
The draws below stay inside these ranges and needn't reach their ends.
All inputs are finite; a program needn't handle non-finite values.
Results may differ from the reference program's by a relative error of at most 0.007.
Values may be sent and summed in bfloat16 or wider, within the bound.
No kernel may reach another device: no remote copies, remote signals or barrier semaphores. Data moves between devices by JAX's collectives and lax.ppermute only.
A program may use at most 64 MiB of HBM per device.

```python
import jax
import jax.numpy as jnp
from jax import lax

N = 512
D = 256
K = 32
B = 256


def draw_embeddings(key, part):
    noise_key = jax.random.fold_in(key, 11)
    sample_key = jax.random.fold_in(key, 12)
    position = jnp.arange(N, dtype=jnp.float32) / jnp.float32(max(N - 1, 1))
    sample_scale = jnp.exp(jax.random.uniform(sample_key, (B,), jnp.float32, jnp.log(0.5), jnp.log(2.0)))
    noise = jnp.clip(jax.random.normal(noise_key, (N, B, D), jnp.float32), -6.0, 6.0)
    offset = 0.3 * jnp.exp(position * jnp.log(3.0))
    values = noise + offset[:, None, None] * sample_scale[None, :, None]
    return values.astype(jnp.bfloat16)


def level_of(rng, dims, pieces, smallest, top_value):
    def one(dim, blocks):
        heights = jax.random.uniform(jax.random.fold_in(jax.random.fold_in(rng, 6), dim), (blocks,), jnp.float32, smallest / len(pieces), top_value / len(pieces))
        return jnp.repeat(jnp.exp(heights), dims[dim] // blocks).reshape((-1,) + (1,) * (len(dims) - dim - 1))

    gain = one(*pieces[0])
    for cut in pieces[1:]:
        gain = gain * one(*cut)
    return gain


def gaussian(stream_key, dims, scale, bound, pieces=(), held_as=jnp.bfloat16):
    drawn = scale * jax.random.normal(stream_key, dims, jnp.float32)
    if pieces:
        drawn = drawn * level_of(stream_key, dims, pieces, -0.22, 0.18)
    return jnp.clip(drawn, -bound, bound).astype(held_as)


def setup_inputs(seed: int = 0) -> dict:
    key_list = jax.random.split(jax.random.key(seed), 7)
    embeddings = draw_embeddings(jax.random.fold_in(key_list[6], 71), 0)
    machine_projection = gaussian(key_list[1], (N, K), (N * D) ** -0.5, 0.015625)
    w_lcb = gaussian(key_list[2], (N, N), N ** -0.5, 0.25, ((0, 4),))
    w_fmb = gaussian(key_list[3], (K, D), K ** -0.5, 1.0)
    ln_gain = jnp.clip(1.0 + 0.1 * jax.random.normal(key_list[4], (N, D), jnp.float32), 0.5, 1.5)
    ln_bias = gaussian(key_list[5], (N, D), 0.3, 1.8, ((0, 8),), jnp.float32)
    return dict(embeddings=embeddings, machine_projection=machine_projection, w_lcb=w_lcb, w_fmb=w_fmb, ln_gain=ln_gain, ln_bias=ln_bias)


def reference(embeddings, machine_projection, w_lcb, w_fmb, ln_gain, ln_bias):
    emb_count, samples, width = embeddings.shape
    factor_dimension = machine_projection.shape[1]
    compressed = jnp.dot(w_lcb, embeddings.reshape(emb_count, samples * width), preferred_element_type=jnp.float32).reshape(emb_count, samples, width)
    widened_inputs = embeddings.astype(jnp.float32)
    summed_values = jnp.einsum('slc,sf->lfc', widened_inputs, machine_projection.astype(jnp.float32))
    factor_matrix = summed_values.astype(jnp.bfloat16)
    inner_product = jnp.einsum('gue,ufe->guf', widened_inputs, factor_matrix.astype(jnp.float32)).astype(jnp.bfloat16)
    fmb_out = jnp.dot(inner_product.reshape(emb_count * samples, factor_dimension), w_fmb, preferred_element_type=jnp.float32).reshape(emb_count, samples, width)
    mixed = widened_inputs + compressed + fmb_out
    entries = jnp.float32(emb_count * width)
    average = lax.optimization_barrier(jnp.sum(mixed, axis=(0, 2))) / entries
    centered = mixed - average[None, :, None]
    spread = lax.optimization_barrier(jnp.sum(centered * centered, axis=(0, 2))) / entries
    scaled = centered * jax.lax.rsqrt(spread + 1e-05)[None, :, None]
    return (scaled * ln_gain[:, None, :] + ln_bias[:, None, :]).astype(jnp.bfloat16)
```

```python
import functools

import jax
import jax.numpy as jnp
from jax import lax
from jax.experimental import pallas as pl
from jax.experimental.pallas import tpu as pltpu
from jax.sharding import PartitionSpec as P


GROUP = 8
EPS = 1e-05


def target(me, m, count):
    if count & (count - 1) == 0:
        return me ^ m
    return lax.rem(me + m, count)


def origin(me, m, count):
    if count & (count - 1) == 0:
        return me ^ m
    return lax.rem(me + count - m, count)


def send(value, m, axis, count, back=False):
    if m == 0:
        return value
    pairs = []
    for i in range(count):
        j = i ^ m if count & (count - 1) == 0 else (i + m) % count
        pairs.append((j, i) if back else (i, j))
    return lax.ppermute(value, axis, pairs)


def row_block(rows):
    size = 32
    while rows % size:
        size //= 2
    return size


def pick_matrix(height, width, inner_out, inner_in):
    i = lax.broadcasted_iota(jnp.int32, (height, width), 0)
    j = lax.broadcasted_iota(jnp.int32, (height, width), 1)
    hit = (i // inner_out == j % inner_in) & (i % inner_out == j // inner_in)
    return jnp.where(hit, 1.0, 0.0).astype(jnp.bfloat16)


def split_kernel(messages, chunks, count, x_ref, *refs):
    outs = refs[: len(messages)]
    landed, sems = refs[len(messages) :]
    rows, _, width = x_ref.shape
    me = lax.axis_index("emb")
    distinct = sorted({m for m, _ in messages}, key=[m for m, _ in messages].index)

    def fetch(k):
        first = pl.multiple_of(target(me, distinct[k], count) * GROUP, GROUP)
        return pltpu.make_async_copy(x_ref.at[:, pl.ds(first, GROUP), :], landed.at[k], sems.at[k])

    for k in range(len(distinct)):
        fetch(k).start()
    block = row_block(rows)
    part = GROUP // chunks
    pick = pick_matrix(GROUP * block, block * GROUP, block, GROUP)
    for k, m in enumerate(distinct):
        fetch(k).wait()
        for q, (m2, c) in enumerate(messages):
            if m2 != m:
                continue
            for b in range(rows // block):
                piece = landed[k, b * block : (b + 1) * block].reshape(block * GROUP, width)
                moved = jnp.dot(
                    pick[c * part * block : (c + 1) * part * block], piece, preferred_element_type=jnp.float32
                )
                outs[q][:, b * block : (b + 1) * block, :] = moved.astype(jnp.bfloat16).reshape(part, block, width)


def split(x, messages, chunks, count):
    rows, samples, width = x.shape
    part = GROUP // chunks
    distinct = len({m for m, _ in messages})
    out = jax.ShapeDtypeStruct((part, rows, width), jnp.bfloat16)
    return pl.pallas_call(
        functools.partial(split_kernel, messages, chunks, count),
        out_shape=[out] * len(messages),
        in_specs=[pl.BlockSpec(memory_space=pl.ANY)],
        out_specs=[pl.BlockSpec(memory_space=pltpu.VMEM)] * len(messages),
        scratch_shapes=[
            pltpu.VMEM((distinct, rows, GROUP, width), jnp.bfloat16),
            pltpu.SemaphoreType.DMA((distinct,)),
        ],
        compiler_params=pltpu.CompilerParams(vmem_limit_bytes=24 * 1024 * 1024),
        cost_estimate=pl.CostEstimate(flops=10**8, bytes_accessed=10**6, transcendentals=0),
        name="split",
    )(x)


def merge_kernel(messages, chunks, count, first, *refs):
    pieces = refs[: len(messages) * chunks]
    gain_ref, bias_ref = refs[len(messages) * chunks : len(messages) * chunks + 2]
    rest = refs[len(messages) * chunks + 2 :]
    out_ref, ready, sems = rest if first else rest[1:]
    part, rows, width = pieces[0].shape
    me = lax.axis_index("emb")
    block = row_block(rows)
    pick = pick_matrix(block * GROUP, GROUP * block, GROUP, block)
    copies = []
    for k, m in enumerate(messages):
        for b in range(rows // block):
            here = slice(b * block, (b + 1) * block)
            gain, bias = gain_ref[here], bias_ref[here]
            done = [
                (pieces[k * chunks + c][:, here, :].astype(jnp.float32) * gain[None] + bias[None]).astype(jnp.bfloat16)
                for c in range(chunks)
            ]
            done = jnp.concatenate(done, axis=0).reshape(GROUP * block, width)
            moved = jnp.dot(pick, done, preferred_element_type=jnp.float32)
            ready[k, here] = moved.astype(jnp.bfloat16).reshape(block, GROUP, width)
        start = pl.multiple_of(target(me, m, count) * GROUP, GROUP)
        copies.append(pltpu.make_async_copy(ready.at[k], out_ref.at[:, pl.ds(start, GROUP), :], sems.at[k]))
        copies[-1].start()
    for copy in copies:
        copy.wait()


def merge(out, pieces, gain, bias, messages, chunks, count, samples):
    part, rows, width = pieces[0].shape
    first = out is None
    vmem = pl.BlockSpec(memory_space=pltpu.VMEM)
    hbm = pl.BlockSpec(memory_space=pl.ANY)
    operands = list(pieces) + [gain, bias] + ([] if first else [out])
    return pl.pallas_call(
        functools.partial(merge_kernel, messages, chunks, count, first),
        out_shape=jax.ShapeDtypeStruct((rows, samples, width), jnp.bfloat16),
        in_specs=[vmem] * (len(pieces) + 2) + ([] if first else [hbm]),
        out_specs=hbm,
        input_output_aliases={} if first else {len(operands) - 1: 0},
        scratch_shapes=[
            pltpu.VMEM((len(messages), rows, GROUP, width), jnp.bfloat16),
            pltpu.SemaphoreType.DMA((len(messages),)),
        ],
        compiler_params=pltpu.CompilerParams(vmem_limit_bytes=24 * 1024 * 1024),
        cost_estimate=pl.CostEstimate(flops=10**8, bytes_accessed=10**6, transcendentals=0),
        name="merge",
    )(*operands)


def layer_kernel(count, pieces_w, *refs):
    blocks = refs[:count]
    weights = refs[count : count + pieces_w]
    proj_ref, fmb_ref = refs[count + pieces_w : count + pieces_w + 2]
    outs = refs[count + pieces_w + 2 : count + pieces_w + 2 + count]
    full_w, held, mixed = refs[count + pieces_w + 2 + count :]
    part, rows, width = blocks[0].shape
    total = count * rows
    me = lax.axis_index("emb")
    mine = lax.axis_index("dp")
    share_w = weights[0].shape[0]
    for q in range(pieces_w):
        full_w[pl.ds(pl.multiple_of(origin(mine, q, pieces_w) * share_w, share_w), share_w), :] = weights[q][...]
    entries = float(total * width)
    starts = [pl.multiple_of(origin(me, m, count) * rows, rows) for m in range(count)]

    def one(s, _):
        for m in range(count):
            held[pl.ds(starts[m], rows), :] = blocks[m][s]
        x = held[...]
        summed = lax.dot_general(proj_ref[...], x, (((0,), (0,)), ((), ())), preferred_element_type=jnp.float32)
        factor = summed.astype(jnp.bfloat16)
        inner = lax.dot_general(x, factor, (((1,), (1,)), ((), ())), preferred_element_type=jnp.float32)
        fmb = jnp.dot(inner.astype(jnp.bfloat16), fmb_ref[...], preferred_element_type=jnp.float32)
        compressed = jnp.dot(full_w[...], x, preferred_element_type=jnp.float32)
        value = x.astype(jnp.float32) + compressed + fmb
        mixed[...] = value
        average = jnp.sum(value) / entries
        centered = mixed[...] - average
        spread = jnp.sum(centered * centered) / entries
        scale = lax.rsqrt(jnp.full((1, width), spread + EPS, jnp.float32))
        for m in range(count):
            outs[m][s] = ((mixed[pl.ds(starts[m], rows), :] - average) * scale).astype(jnp.bfloat16)
        return 0

    lax.fori_loop(0, part, one, 0)


def layer(blocks, weights, proj, w_fmb):
    part, rows, width = blocks[0].shape
    count = len(blocks)
    total = count * rows
    vmem = pl.BlockSpec(memory_space=pltpu.VMEM)
    return pl.pallas_call(
        functools.partial(layer_kernel, count, len(weights)),
        out_shape=[jax.ShapeDtypeStruct((part, rows, width), jnp.bfloat16)] * count,
        in_specs=[vmem] * (count + len(weights) + 2),
        out_specs=[vmem] * count,
        scratch_shapes=[
            pltpu.VMEM((weights[0].shape[0] * len(weights), total), jnp.bfloat16),
            pltpu.VMEM((total, width), jnp.bfloat16),
            pltpu.VMEM((total, width), jnp.float32),
        ],
        compiler_params=pltpu.CompilerParams(vmem_limit_bytes=24 * 1024 * 1024),
        cost_estimate=pl.CostEstimate(
            flops=2 * part * total * total * width, bytes_accessed=4 * part * total * width, transcendentals=0
        ),
        name="layer",
    )(*blocks, *weights, proj, w_fmb)


def body(embeddings, machine_projection, w_lcb, w_fmb, ln_gain, ln_bias):
    rows, samples, width = embeddings.shape
    count = lax.axis_size("emb")
    others = lax.axis_size("dp")
    share = samples // count
    chunks = 2 if share % 2 == 0 else 1
    part = share // chunks
    far = [m for m in range(count) if m >= count // 2]
    near = [m for m in range(1, count) if m < count // 2]
    fast = share == GROUP
    sends = {}

    if fast:

        def cut(names):
            sends.update(zip(names, split(embeddings, names, chunks, count)))

    else:
        turned = embeddings.reshape(rows, count, chunks, part, width).transpose(1, 2, 3, 0, 4)
        me = lax.axis_index("emb")

        def cut(names):
            for m, c in names:
                sends[m, c] = lax.dynamic_index_in_dim(turned, target(me, m, count), 0, keepdims=False)[c]

    arrived = {}

    def forward(names):
        for m, c in names:
            arrived[m, c] = send(sends[m, c], m, "emb", count)

    cut([(m, 0) for m in far])
    forward([(m, 0) for m in far])
    cut([(m, 0) for m in near] + [(0, 0)] + [(m, c) for c in range(1, chunks) for m in far + near + [0]])
    forward([(m, 0) for m in near + [0]])
    weights = [send(w_lcb, q, "dp", others) for q in range(others)]
    for c in range(1, chunks):
        forward([(m, c) for m in far + near + [0]])

    returned = {}
    for c in range(chunks):
        done = layer([arrived[m, c] for m in range(count)], weights, machine_projection, w_fmb)
        for m in near + far + [0]:
            returned[m, c] = send(done[m], m, "emb", count, back=True)

    if fast:
        out = None
        for messages in [[0] + near] + [[m] for m in far]:
            pieces = [returned[m, c] for m in messages for c in range(chunks)]
            out = merge(out, pieces, ln_gain, ln_bias, messages, chunks, count, samples)
        return out
    me = lax.axis_index("emb")
    stacked = jnp.stack([jnp.concatenate([returned[m, c] for c in range(chunks)]) for m in range(count)])
    finished = (stacked.astype(jnp.float32) * ln_gain + ln_bias).astype(jnp.bfloat16)
    order = jnp.stack([_message_to(me, j, count) for j in range(count)])
    finished = jnp.take(finished, order, axis=0)
    return finished.transpose(2, 0, 1, 3).reshape(rows, samples, width)


def _message_to(me, j, count):
    if count & (count - 1) == 0:
        return me ^ j
    return lax.rem(j - me + count, count)


def solution(mesh):
    return jax.shard_map(
        body,
        mesh=mesh,
        in_specs=(P("emb", "dp", None), P(), P("dp", None), P(), P("emb", None), P("emb", None)),
        out_specs=P("emb", "dp", None),
        check_vma=False,
    )
```

```python
import functools

import jax
import jax.numpy as jnp
from jax import lax
from jax.experimental import pallas as pl
from jax.experimental.pallas import tpu as pltpu
from jax.sharding import PartitionSpec as P


GROUP = 8
EPS = 1e-05


def target(me, m, count):
    if count & (count - 1) == 0:
        return me ^ m
    return lax.rem(me + m, count)


def origin(me, m, count):
    if count & (count - 1) == 0:
        return me ^ m
    return lax.rem(me + count - m, count)


def send(value, m, axis, count, back=False):
    if m == 0:
        return value
    pairs = []
    for i in range(count):
        j = i ^ m if count & (count - 1) == 0 else (i + m) % count
        pairs.append((j, i) if back else (i, j))
    return lax.ppermute(value, axis, pairs)


def row_block(rows):
    size = 32
    while rows % size:
        size //= 2
    return size


def pick_matrix(height, width, inner_out, inner_in):
    i = lax.broadcasted_iota(jnp.int32, (height, width), 0)
    j = lax.broadcasted_iota(jnp.int32, (height, width), 1)
    hit = (i // inner_out == j % inner_in) & (i % inner_out == j // inner_in)
    return jnp.where(hit, 1.0, 0.0).astype(jnp.bfloat16)


def split_kernel(messages, chunks, count, x_ref, *refs):
    outs = refs[: len(messages)]
    landed, sems = refs[len(messages) :]
    rows, _, width = x_ref.shape
    me = lax.axis_index("emb")
    distinct = sorted({m for m, _ in messages}, key=[m for m, _ in messages].index)

    def fetch(k):
        first = pl.multiple_of(target(me, distinct[k], count) * GROUP, GROUP)
        return pltpu.make_async_copy(x_ref.at[:, pl.ds(first, GROUP), :], landed.at[k], sems.at[k])

    for k in range(len(distinct)):
        fetch(k).start()
    block = row_block(rows)
    part = GROUP // chunks
    pick = pick_matrix(GROUP * block, block * GROUP, block, GROUP)
    for k, m in enumerate(distinct):
        fetch(k).wait()
        for q, (m2, c) in enumerate(messages):
            if m2 != m:
                continue
            for b in range(rows // block):
                piece = landed[k, b * block : (b + 1) * block].reshape(block * GROUP, width)
                moved = jnp.dot(
                    pick[c * part * block : (c + 1) * part * block], piece, preferred_element_type=jnp.float32
                )
                outs[q][:, b * block : (b + 1) * block, :] = moved.astype(jnp.bfloat16).reshape(part, block, width)


def split(x, messages, chunks, count):
    rows, _, width = x.shape
    part = GROUP // chunks
    distinct = len({m for m, _ in messages})
    out = jax.ShapeDtypeStruct((part, rows, width), jnp.bfloat16)
    return pl.pallas_call(
        functools.partial(split_kernel, messages, chunks, count),
        out_shape=[out] * len(messages),
        in_specs=[pl.BlockSpec(memory_space=pltpu.HBM)],
        out_specs=[pl.BlockSpec(memory_space=pltpu.VMEM)] * len(messages),
        scratch_shapes=[
            pltpu.VMEM((distinct, rows, GROUP, width), jnp.bfloat16),
            pltpu.SemaphoreType.DMA((distinct,)),
        ],
        compiler_params=pltpu.CompilerParams(vmem_limit_bytes=12 * 1024 * 1024),
        cost_estimate=pl.CostEstimate(flops=10**8, bytes_accessed=10**6, transcendentals=0),
        name="split",
    )(x)


def merge_kernel(messages, chunks, count, first, *refs):
    pieces = refs[: len(messages) * chunks]
    gain_ref, bias_ref = refs[len(messages) * chunks : len(messages) * chunks + 2]
    rest = refs[len(messages) * chunks + 2 :]
    out_ref, ready, sems = rest if first else rest[1:]
    _, rows, width = pieces[0].shape
    me = lax.axis_index("emb")
    block = row_block(rows)
    pick = pick_matrix(block * GROUP, GROUP * block, GROUP, block)
    copies = []
    for k, m in enumerate(messages):
        for b in range(rows // block):
            here = slice(b * block, (b + 1) * block)
            gain, bias = gain_ref[here], bias_ref[here]
            done = [
                (pieces[k * chunks + c][:, here, :].astype(jnp.float32) * gain[None] + bias[None]).astype(jnp.bfloat16)
                for c in range(chunks)
            ]
            done = jnp.concatenate(done, axis=0).reshape(GROUP * block, width)
            moved = jnp.dot(pick, done, preferred_element_type=jnp.float32)
            ready[k, here] = moved.astype(jnp.bfloat16).reshape(block, GROUP, width)
        start = pl.multiple_of(target(me, m, count) * GROUP, GROUP)
        copies.append(pltpu.make_async_copy(ready.at[k], out_ref.at[:, pl.ds(start, GROUP), :], sems.at[k]))
        copies[-1].start()
    for copy in copies:
        copy.wait()


def merge(out, pieces, gain, bias, messages, chunks, count, samples):
    _, rows, width = pieces[0].shape
    first = out is None
    vmem = pl.BlockSpec(memory_space=pltpu.VMEM)
    hbm = pl.BlockSpec(memory_space=pl.ANY)
    operands = list(pieces) + [gain, bias] + ([] if first else [out])
    return pl.pallas_call(
        functools.partial(merge_kernel, messages, chunks, count, first),
        out_shape=jax.ShapeDtypeStruct((rows, samples, width), jnp.bfloat16),
        in_specs=[vmem] * (len(pieces) + 2) + ([] if first else [hbm]),
        out_specs=hbm,
        input_output_aliases={} if first else {len(operands) - 1: 0},
        scratch_shapes=[
            pltpu.VMEM((len(messages), rows, GROUP, width), jnp.bfloat16),
            pltpu.SemaphoreType.DMA((len(messages),)),
        ],
        compiler_params=pltpu.CompilerParams(vmem_limit_bytes=12 * 1024 * 1024),
        cost_estimate=pl.CostEstimate(flops=10**8, bytes_accessed=10**6, transcendentals=0),
        name="merge",
    )(*operands)


def layer_kernel(count, pieces_w, *refs):
    blocks = refs[:count]
    weights = refs[count : count + pieces_w]
    proj_ref, fmb_ref = refs[count + pieces_w : count + pieces_w + 2]
    outs = refs[count + pieces_w + 2 : count + pieces_w + 2 + count]
    full_w, held, mixed = refs[count + pieces_w + 2 + count :]
    part, rows, width = blocks[0].shape
    total = count * rows
    me = lax.axis_index("emb")
    mine = lax.axis_index("dp")
    share_w = weights[0].shape[0]
    for q in range(pieces_w):
        full_w[pl.ds(pl.multiple_of(origin(mine, q, pieces_w) * share_w, share_w), share_w), :] = weights[q][...]
    entries = float(total * width)
    starts = [pl.multiple_of(origin(me, m, count) * rows, rows) for m in range(count)]

    def one(s, _):
        for m in range(count):
            held[pl.ds(starts[m], rows), :] = blocks[m][s]
        x = held[...]
        summed = lax.dot_general(proj_ref[...], x, (((0,), (0,)), ((), ())), preferred_element_type=jnp.float32)
        factor = summed.astype(jnp.bfloat16)
        inner = lax.dot_general(x, factor, (((1,), (1,)), ((), ())), preferred_element_type=jnp.float32)
        fmb = jnp.dot(inner.astype(jnp.bfloat16), fmb_ref[...], preferred_element_type=jnp.float32)
        compressed = jnp.dot(full_w[...], x, preferred_element_type=jnp.float32)
        value = x.astype(jnp.float32) + compressed + fmb
        mixed[...] = value
        average = jnp.sum(value) / entries
        centered = mixed[...] - average
        spread = jnp.sum(centered * centered) / entries
        scale = lax.rsqrt(jnp.full((1, width), spread + EPS, jnp.float32))
        for m in range(count):
            outs[m][s] = ((mixed[pl.ds(starts[m], rows), :] - average) * scale).astype(jnp.bfloat16)
        return 0

    lax.fori_loop(0, part, one, 0)


def layer(blocks, weights, proj, w_fmb):
    part, rows, width = blocks[0].shape
    count = len(blocks)
    total = count * rows
    vmem = pl.BlockSpec(memory_space=pltpu.VMEM)
    return pl.pallas_call(
        functools.partial(layer_kernel, count, len(weights)),
        out_shape=[jax.ShapeDtypeStruct((part, rows, width), jnp.bfloat16)] * count,
        in_specs=[vmem] * (count + len(weights) + 2),
        out_specs=[vmem] * count,
        scratch_shapes=[
            pltpu.VMEM((weights[0].shape[0] * len(weights), total), jnp.bfloat16),
            pltpu.VMEM((total, width), jnp.bfloat16),
            pltpu.VMEM((total, width), jnp.float32),
        ],
        compiler_params=pltpu.CompilerParams(vmem_limit_bytes=12 * 1024 * 1024),
        cost_estimate=pl.CostEstimate(
            flops=2 * part * total * total * width, bytes_accessed=4 * part * total * width, transcendentals=0
        ),
        name="layer",
    )(*blocks, *weights, proj, w_fmb)


def body(embeddings, machine_projection, w_lcb, w_fmb, ln_gain, ln_bias):
    rows, samples, width = embeddings.shape
    count = lax.axis_size("emb")
    others = lax.axis_size("dp")
    share = samples // count
    chunks = 2 if share % 2 == 0 else 1
    part = share // chunks
    far = [m for m in range(count) if m >= count // 2]
    near = [m for m in range(1, count) if m < count // 2]
    fast = share == GROUP
    sends = {}

    if fast:

        def cut(names):
            sends.update(zip(names, split(embeddings, names, chunks, count)))

    else:
        turned = embeddings.reshape(rows, count, chunks, part, width).transpose(1, 2, 3, 0, 4)
        me = lax.axis_index("emb")

        def cut(names):
            for m, c in names:
                sends[m, c] = lax.dynamic_index_in_dim(turned, target(me, m, count), 0, keepdims=False)[c]

    arrived = {}

    def forward(names):
        for m, c in names:
            arrived[m, c] = send(sends[m, c], m, "emb", count)

    cut([(m, 0) for m in far])
    forward([(m, 0) for m in far])
    cut([(m, 0) for m in near] + [(0, 0)] + [(m, c) for c in range(1, chunks) for m in far + near + [0]])
    forward([(m, 0) for m in near + [0]])
    weights = []
    for q in range(others):
        weights.append(send(w_lcb, q, "dp", others))
    for c in range(1, chunks):
        forward([(m, c) for m in far + near + [0]])

    returned = {}
    for c in range(chunks):
        done = layer([arrived[m, c] for m in range(count)], weights, machine_projection, w_fmb)
        for m in near + far + [0]:
            returned[m, c] = send(done[m], m, "emb", count, back=True)

    if fast:
        out = None
        for messages in [[0] + near] + [[m] for m in far]:
            pieces = [returned[m, c] for m in messages for c in range(chunks)]
            out = merge(out, pieces, ln_gain, ln_bias, messages, chunks, count, samples)
        return out
    me = lax.axis_index("emb")
    stacked = jnp.stack([jnp.concatenate([returned[m, c] for c in range(chunks)]) for m in range(count)])
    finished = (stacked.astype(jnp.float32) * ln_gain + ln_bias).astype(jnp.bfloat16)
    order = jnp.stack([_message_to(me, j, count) for j in range(count)])
    finished = jnp.take(finished, order, axis=0)
    return finished.transpose(2, 0, 1, 3).reshape(rows, samples, width)


def _message_to(me, j, count):
    if count & (count - 1) == 0:
        return me ^ j
    return lax.rem(j - me + count, count)


def solution(mesh):
    return jax.shard_map(
        body,
        mesh=mesh,
        in_specs=(P("emb", "dp", None), P(), P("dp", None), P(), P("emb", None), P("emb", None)),
        out_specs=P("emb", "dp", None),
        check_vma=False,
    )
```

```python
import functools

import jax
import jax.numpy as jnp
from jax import lax
from jax.experimental import pallas as pl
from jax.experimental.pallas import tpu as pltpu
from jax.sharding import PartitionSpec as P


GROUP = 8
EPS = 1e-05


def target(me, m, count):
    if count & (count - 1) == 0:
        return me ^ m
    return lax.rem(me + m, count)


def origin(me, m, count):
    if count & (count - 1) == 0:
        return me ^ m
    return lax.rem(me + count - m, count)


def send(value, m, axis, count, back=False):
    if m == 0:
        return value
    pairs = []
    for i in range(count):
        j = i ^ m if count & (count - 1) == 0 else (i + m) % count
        pairs.append((j, i) if back else (i, j))
    return lax.ppermute(value, axis, pairs)


def row_block(rows):
    size = 32
    while rows % size:
        size //= 2
    return size


def pick_matrix(height, width, inner_out, inner_in):
    i = lax.broadcasted_iota(jnp.int32, (height, width), 0)
    j = lax.broadcasted_iota(jnp.int32, (height, width), 1)
    hit = (i // inner_out == j % inner_in) & (i % inner_out == j // inner_in)
    return jnp.where(hit, 1.0, 0.0).astype(jnp.bfloat16)


def split_kernel(messages, chunks, count, x_ref, *refs):
    outs = refs[: len(messages)]
    landed, sems = refs[len(messages) :]
    rows, _, width = x_ref.shape
    me = lax.axis_index("emb")
    distinct = sorted({m for m, _ in messages}, key=[m for m, _ in messages].index)

    def fetch(k):
        first = pl.multiple_of(target(me, distinct[k], count) * GROUP, GROUP)
        return pltpu.make_async_copy(x_ref.at[:, pl.ds(first, GROUP), :], landed.at[k], sems.at[k])

    for k in range(len(distinct)):
        fetch(k).start()
    block = row_block(rows)
    part = GROUP // chunks
    pick = pick_matrix(GROUP * block, block * GROUP, block, GROUP)
    for k, m in enumerate(distinct):
        fetch(k).wait()
        for q, (m2, c) in enumerate(messages):
            if m2 != m:
                continue
            for b in range(rows // block):
                piece = landed[k, b * block : (b + 1) * block].reshape(block * GROUP, width)
                moved = jnp.dot(
                    pick[c * part * block : (c + 1) * part * block], piece, preferred_element_type=jnp.float32
                )
                outs[q][:, b * block : (b + 1) * block, :] = moved.astype(jnp.bfloat16).reshape(part, block, width)


def split(x, messages, chunks, count, first):
    rows, _, width = x.shape
    part = GROUP // chunks
    distinct = len({m for m, _ in messages})
    out = jax.ShapeDtypeStruct((part, rows, width), jnp.bfloat16)
    return pl.pallas_call(
        functools.partial(split_kernel, messages, chunks, count),
        out_shape=[out] * len(messages),
        in_specs=[pl.BlockSpec(memory_space=pltpu.HBM)],
        out_specs=[pl.BlockSpec(memory_space=pltpu.VMEM)] * len(messages),
        scratch_shapes=[
            pltpu.VMEM((distinct, rows, GROUP, width), jnp.bfloat16),
            pltpu.SemaphoreType.DMA((distinct,)),
        ],
        compiler_params=pltpu.CompilerParams(vmem_limit_bytes=12 * 1024 * 1024),
        cost_estimate=pl.CostEstimate(flops=10**8, bytes_accessed=10**6, transcendentals=0),
        name="split",
    )(pltpu.with_memory_space_constraint(x, pltpu.HBM) if first else x)


def merge_kernel(messages, chunks, count, first, *refs):
    pieces = refs[: len(messages) * chunks]
    gain_ref, bias_ref = refs[len(messages) * chunks : len(messages) * chunks + 2]
    rest = refs[len(messages) * chunks + 2 :]
    out_ref, ready, sems = rest if first else rest[1:]
    _, rows, width = pieces[0].shape
    me = lax.axis_index("emb")
    block = row_block(rows)
    pick = pick_matrix(block * GROUP, GROUP * block, GROUP, block)
    copies = []
    for k, m in enumerate(messages):
        for b in range(rows // block):
            here = slice(b * block, (b + 1) * block)
            gain, bias = gain_ref[here], bias_ref[here]
            done = [
                (pieces[k * chunks + c][:, here, :].astype(jnp.float32) * gain[None] + bias[None]).astype(jnp.bfloat16)
                for c in range(chunks)
            ]
            done = jnp.concatenate(done, axis=0).reshape(GROUP * block, width)
            moved = jnp.dot(pick, done, preferred_element_type=jnp.float32)
            ready[k, here] = moved.astype(jnp.bfloat16).reshape(block, GROUP, width)
        start = pl.multiple_of(target(me, m, count) * GROUP, GROUP)
        copies.append(pltpu.make_async_copy(ready.at[k], out_ref.at[:, pl.ds(start, GROUP), :], sems.at[k]))
        copies[-1].start()
    for copy in copies:
        copy.wait()


def merge(out, pieces, gain, bias, messages, chunks, count, samples):
    _, rows, width = pieces[0].shape
    first = out is None
    vmem = pl.BlockSpec(memory_space=pltpu.VMEM)
    hbm = pl.BlockSpec(memory_space=pl.ANY)
    operands = list(pieces) + [gain, bias] + ([] if first else [out])
    return pl.pallas_call(
        functools.partial(merge_kernel, messages, chunks, count, first),
        out_shape=jax.ShapeDtypeStruct((rows, samples, width), jnp.bfloat16),
        in_specs=[vmem] * (len(pieces) + 2) + ([] if first else [hbm]),
        out_specs=hbm,
        input_output_aliases={} if first else {len(operands) - 1: 0},
        scratch_shapes=[
            pltpu.VMEM((len(messages), rows, GROUP, width), jnp.bfloat16),
            pltpu.SemaphoreType.DMA((len(messages),)),
        ],
        compiler_params=pltpu.CompilerParams(vmem_limit_bytes=12 * 1024 * 1024),
        cost_estimate=pl.CostEstimate(flops=10**8, bytes_accessed=10**6, transcendentals=0),
        name="merge",
    )(*operands)


def layer_kernel(count, pieces_w, *refs):
    blocks = refs[:count]
    weights = refs[count : count + pieces_w]
    proj_ref, fmb_ref = refs[count + pieces_w : count + pieces_w + 2]
    outs = refs[count + pieces_w + 2 : count + pieces_w + 2 + count]
    full_w, held, mixed = refs[count + pieces_w + 2 + count :]
    part, rows, width = blocks[0].shape
    total = count * rows
    me = lax.axis_index("emb")
    mine = lax.axis_index("dp")
    share_w = weights[0].shape[0]
    for q in range(pieces_w):
        full_w[pl.ds(pl.multiple_of(origin(mine, q, pieces_w) * share_w, share_w), share_w), :] = weights[q][...]
    entries = float(total * width)
    starts = [pl.multiple_of(origin(me, m, count) * rows, rows) for m in range(count)]

    def one(s, _):
        for m in range(count):
            held[pl.ds(starts[m], rows), :] = blocks[m][s]
        x = held[...]
        summed = jnp.dot(proj_ref[...], x, preferred_element_type=jnp.float32)
        factor = summed.astype(jnp.bfloat16)
        inner = lax.dot_general(x, factor, (((1,), (1,)), ((), ())), preferred_element_type=jnp.float32)
        fmb = jnp.dot(inner.astype(jnp.bfloat16), fmb_ref[...], preferred_element_type=jnp.float32)
        compressed = jnp.dot(full_w[...], x, preferred_element_type=jnp.float32)
        value = x.astype(jnp.float32) + compressed + fmb
        mixed[...] = value
        average = jnp.sum(value) / entries
        centered = mixed[...] - average
        spread = jnp.sum(centered * centered) / entries
        scale = lax.rsqrt(jnp.full((1, width), spread + EPS, jnp.float32))
        for m in range(count):
            outs[m][s] = ((mixed[pl.ds(starts[m], rows), :] - average) * scale).astype(jnp.bfloat16)
        return 0

    lax.fori_loop(0, part, one, 0)


def layer(blocks, weights, proj, w_fmb):
    part, rows, width = blocks[0].shape
    count = len(blocks)
    total = count * rows
    vmem = pl.BlockSpec(memory_space=pltpu.VMEM)
    return pl.pallas_call(
        functools.partial(layer_kernel, count, len(weights)),
        out_shape=[jax.ShapeDtypeStruct((part, rows, width), jnp.bfloat16)] * count,
        in_specs=[vmem] * (count + len(weights) + 2),
        out_specs=[vmem] * count,
        scratch_shapes=[
            pltpu.VMEM((weights[0].shape[0] * len(weights), total), jnp.bfloat16),
            pltpu.VMEM((total, width), jnp.bfloat16),
            pltpu.VMEM((total, width), jnp.float32),
        ],
        compiler_params=pltpu.CompilerParams(vmem_limit_bytes=12 * 1024 * 1024),
        cost_estimate=pl.CostEstimate(
            flops=2 * part * total * total * width, bytes_accessed=4 * part * total * width, transcendentals=0
        ),
        name="layer",
    )(*blocks, *weights, proj, w_fmb)


def body(embeddings, machine_projection, w_lcb, w_fmb, ln_gain, ln_bias):
    rows, samples, width = embeddings.shape
    count = lax.axis_size("emb")
    others = lax.axis_size("dp")
    share = samples // count
    chunks = 2 if share % 2 == 0 else 1
    part = share // chunks
    far = [m for m in range(count - 1, 0, -1) if m >= count // 2]
    near = [m for m in range(1, count) if m < count // 2]
    fast = share == GROUP
    sends = {}

    if fast:

        def cut(names):
            sends.update(zip(names, split(embeddings, names, chunks, count, not sends)))

    else:
        turned = embeddings.reshape(rows, count, chunks, part, width).transpose(1, 2, 3, 0, 4)
        me = lax.axis_index("emb")

        def cut(names):
            for m, c in names:
                sends[m, c] = lax.dynamic_index_in_dim(turned, target(me, m, count), 0, keepdims=False)[c]

    arrived = {}

    def forward(names):
        for m, c in names:
            arrived[m, c] = send(sends[m, c], m, "emb", count)

    cut([(m, 0) for m in far[:2]])
    forward([(m, 0) for m in far[:2]])
    cut([(m, 0) for m in far[2:] + near + [0]] + [(m, c) for c in range(1, chunks) for m in far + near + [0]])
    forward([(m, 0) for m in far[2:] + near + [0]])
    weights = []
    for q in range(others):
        weights.append(send(w_lcb, q, "dp", others))
    for c in range(1, chunks):
        forward([(m, c) for m in near + far + [0]])

    returned = {}
    for c in range(chunks):
        done = layer([arrived[m, c] for m in range(count)], weights, machine_projection.T, w_fmb)
        for m in near + far + [0]:
            returned[m, c] = send(done[m], m, "emb", count, back=True)

    if fast:
        out = None
        for messages in [[0] + near] + [[m] for m in far[::-1]]:
            pieces = [returned[m, c] for m in messages for c in range(chunks)]
            out = merge(out, pieces, ln_gain, ln_bias, messages, chunks, count, samples)
        return out
    me = lax.axis_index("emb")
    stacked = jnp.stack([jnp.concatenate([returned[m, c] for c in range(chunks)]) for m in range(count)])
    finished = (stacked.astype(jnp.float32) * ln_gain + ln_bias).astype(jnp.bfloat16)
    order = jnp.stack([_message_to(me, j, count) for j in range(count)])
    finished = jnp.take(finished, order, axis=0)
    return finished.transpose(2, 0, 1, 3).reshape(rows, samples, width)


def _message_to(me, j, count):
    if count & (count - 1) == 0:
        return me ^ j
    return lax.rem(j - me + count, count)


def solution(mesh):
    return jax.shard_map(
        body,
        mesh=mesh,
        in_specs=(P("emb", "dp", None), P(), P("dp", None), P(), P("emb", None), P("emb", None)),
        out_specs=P("emb", "dp", None),
        check_vma=False,
    )
```

```python
import functools

import jax
import jax.numpy as jnp
from jax import lax
from jax.experimental import pallas as pl
from jax.experimental.pallas import tpu as pltpu
from jax.sharding import PartitionSpec as P


GROUP = 8
EPS = 1e-05


def target(me, m, count):
    if count & (count - 1) == 0:
        return me ^ m
    return lax.rem(me + m, count)


def origin(me, m, count):
    if count & (count - 1) == 0:
        return me ^ m
    return lax.rem(me + count - m, count)


def sides(count):
    half = count // 2
    return sorted(range(half, count), key=lambda m: (-(m // 2), m)), list(range(1, half))


def chunk_count(share):
    return 2 if share % 2 == 0 else 1


def send(value, m, axis, count, back=False):
    if m == 0:
        return value
    pairs = []
    for i in range(count):
        j = i ^ m if count & (count - 1) == 0 else (i + m) % count
        pairs.append((j, i) if back else (i, j))
    return lax.ppermute(value, axis, pairs)


def row_block(rows):
    size = 32
    while rows % size:
        size //= 2
    return size


def pick_matrix(height, width, inner_out, inner_in):
    i = lax.broadcasted_iota(jnp.int32, (height, width), 0)
    j = lax.broadcasted_iota(jnp.int32, (height, width), 1)
    hit = (i // inner_out == j % inner_in) & (i % inner_out == j // inner_in)
    return jnp.where(hit, 1.0, 0.0).astype(jnp.bfloat16)


def split_kernel(messages, chunks, count, x_ref, *refs):
    outs = refs[: len(messages)]
    landed, sems = refs[len(messages) :]
    rows, _, width = x_ref.shape
    me = lax.axis_index("emb")
    distinct = sorted({m for m, _ in messages}, key=[m for m, _ in messages].index)

    def fetch(k):
        first = pl.multiple_of(target(me, distinct[k], count) * GROUP, GROUP)
        return pltpu.make_async_copy(x_ref.at[:, pl.ds(first, GROUP), :], landed.at[k], sems.at[k])

    for k in range(len(distinct)):
        fetch(k).start()
    block = row_block(rows)
    part = GROUP // chunks
    pick = pick_matrix(GROUP * block, block * GROUP, block, GROUP)
    for k, m in enumerate(distinct):
        fetch(k).wait()
        for q, (m2, c) in enumerate(messages):
            if m2 != m:
                continue
            for b in range(rows // block):
                piece = landed[k, b * block : (b + 1) * block].reshape(block * GROUP, width)
                moved = jnp.dot(
                    pick[c * part * block : (c + 1) * part * block], piece, preferred_element_type=jnp.float32
                )
                outs[q][:, b * block : (b + 1) * block, :] = moved.astype(jnp.bfloat16).reshape(part, block, width)


def split(x, messages, chunks, count, first):
    rows, _, width = x.shape
    part = GROUP // chunks
    distinct = len({m for m, _ in messages})
    out = jax.ShapeDtypeStruct((part, rows, width), jnp.bfloat16)
    return pl.pallas_call(
        functools.partial(split_kernel, messages, chunks, count),
        out_shape=[out] * len(messages),
        in_specs=[pl.BlockSpec(memory_space=pltpu.HBM)],
        out_specs=[pl.BlockSpec(memory_space=pltpu.VMEM)] * len(messages),
        scratch_shapes=[
            pltpu.VMEM((distinct, rows, GROUP, width), jnp.bfloat16),
            pltpu.SemaphoreType.DMA((distinct,)),
        ],
        compiler_params=pltpu.CompilerParams(vmem_limit_bytes=12 * 1024 * 1024),
        cost_estimate=pl.CostEstimate(flops=10**8, bytes_accessed=10**6, transcendentals=0),
        name="split",
    )(pltpu.with_memory_space_constraint(x, pltpu.HBM) if first else x)


def merge_kernel(messages, chunks, count, first, *refs):
    pieces = refs[: len(messages) * chunks]
    gain_ref, bias_ref = refs[len(messages) * chunks : len(messages) * chunks + 2]
    rest = refs[len(messages) * chunks + 2 :]
    out_ref, ready, sems = rest if first else rest[1:]
    _, rows, width = pieces[0].shape
    me = lax.axis_index("emb")
    block = row_block(rows)
    pick = pick_matrix(block * GROUP, GROUP * block, GROUP, block)
    blocks = rows // block
    copies = []
    for k, m in enumerate(messages):
        start = pl.multiple_of(target(me, m, count) * GROUP, GROUP)
        for b in range(blocks):
            here = slice(b * block, (b + 1) * block)
            gain, bias = gain_ref[here], bias_ref[here]
            done = [
                (pieces[k * chunks + c][:, here, :].astype(jnp.float32) * gain[None] + bias[None]).astype(jnp.bfloat16)
                for c in range(chunks)
            ]
            done = jnp.concatenate(done, axis=0).reshape(GROUP * block, width)
            moved = jnp.dot(pick, done, preferred_element_type=jnp.float32)
            ready[k, here] = moved.astype(jnp.bfloat16).reshape(block, GROUP, width)
            copies.append(
                pltpu.make_async_copy(
                    ready.at[k, here], out_ref.at[here, pl.ds(start, GROUP), :], sems.at[k * blocks + b]
                )
            )
            copies[-1].start()
    for copy in copies:
        copy.wait()


def merge(out, pieces, gain, bias, messages, chunks, count, samples):
    _, rows, width = pieces[0].shape
    first = out is None
    vmem = pl.BlockSpec(memory_space=pltpu.VMEM)
    hbm = pl.BlockSpec(memory_space=pl.ANY)
    operands = list(pieces) + [gain, bias] + ([] if first else [out])
    return pl.pallas_call(
        functools.partial(merge_kernel, messages, chunks, count, first),
        out_shape=jax.ShapeDtypeStruct((rows, samples, width), jnp.bfloat16),
        in_specs=[vmem] * (len(pieces) + 2) + ([] if first else [hbm]),
        out_specs=hbm,
        input_output_aliases={} if first else {len(operands) - 1: 0},
        scratch_shapes=[
            pltpu.VMEM((len(messages), rows, GROUP, width), jnp.bfloat16),
            pltpu.SemaphoreType.DMA((len(messages) * (rows // row_block(rows)),)),
        ],
        compiler_params=pltpu.CompilerParams(vmem_limit_bytes=12 * 1024 * 1024),
        cost_estimate=pl.CostEstimate(flops=10**8, bytes_accessed=10**6, transcendentals=0),
        name="merge",
    )(*operands)


def layer_kernel(count, pieces_w, *refs):
    blocks = refs[:count]
    weights = refs[count : count + pieces_w]
    proj_ref, fmb_ref = refs[count + pieces_w : count + pieces_w + 2]
    outs = refs[count + pieces_w + 2 : count + pieces_w + 2 + count]
    full_w, held, mixed = refs[count + pieces_w + 2 + count :]
    part, rows, width = blocks[0].shape
    total = count * rows
    me = lax.axis_index("emb")
    mine = lax.axis_index("dp")
    share_w = weights[0].shape[0]
    for q in range(pieces_w):
        full_w[pl.ds(pl.multiple_of(origin(mine, q, pieces_w) * share_w, share_w), share_w), :] = weights[q][...]
    entries = float(total * width)
    starts = [pl.multiple_of(origin(me, m, count) * rows, rows) for m in range(count)]

    def one(s, _):
        for m in range(count):
            held[pl.ds(starts[m], rows), :] = blocks[m][s]
        x = held[...]
        summed = jnp.dot(proj_ref[...], x, preferred_element_type=jnp.float32)
        factor = summed.astype(jnp.bfloat16)
        inner = lax.dot_general(x, factor, (((1,), (1,)), ((), ())), preferred_element_type=jnp.float32)
        fmb = jnp.dot(inner.astype(jnp.bfloat16), fmb_ref[...], preferred_element_type=jnp.float32)
        compressed = jnp.dot(full_w[...], x, preferred_element_type=jnp.float32)
        value = x.astype(jnp.float32) + compressed + fmb
        mixed[...] = value
        average = jnp.sum(value) / entries
        centered = mixed[...] - average
        spread = jnp.sum(centered * centered) / entries
        scale = lax.rsqrt(jnp.full((1, width), spread + EPS, jnp.float32))
        for m in range(count):
            outs[m][s] = ((mixed[pl.ds(starts[m], rows), :] - average) * scale).astype(jnp.bfloat16)
        return 0

    lax.fori_loop(0, part, one, 0)


def layer(blocks, weights, proj, w_fmb):
    part, rows, width = blocks[0].shape
    count = len(blocks)
    total = count * rows
    vmem = pl.BlockSpec(memory_space=pltpu.VMEM)
    return pl.pallas_call(
        functools.partial(layer_kernel, count, len(weights)),
        out_shape=[jax.ShapeDtypeStruct((part, rows, width), jnp.bfloat16)] * count,
        in_specs=[vmem] * (count + len(weights) + 2),
        out_specs=[vmem] * count,
        scratch_shapes=[
            pltpu.VMEM((weights[0].shape[0] * len(weights), total), jnp.bfloat16),
            pltpu.VMEM((total, width), jnp.bfloat16),
            pltpu.VMEM((total, width), jnp.float32),
        ],
        compiler_params=pltpu.CompilerParams(vmem_limit_bytes=12 * 1024 * 1024),
        cost_estimate=pl.CostEstimate(
            flops=2 * part * total * total * width, bytes_accessed=4 * part * total * width, transcendentals=0
        ),
        name="layer",
    )(*blocks, *weights, proj, w_fmb)


def body(embeddings, machine_projection, w_lcb, w_fmb, ln_gain, ln_bias):
    rows, samples, width = embeddings.shape
    count = lax.axis_size("emb")
    others = lax.axis_size("dp")
    share = samples // count
    chunks = chunk_count(share)
    part = share // chunks
    far, near = sides(count)
    fast = share == GROUP
    sends = {}

    if fast:

        def cut(names):
            sends.update(zip(names, split(embeddings, names, chunks, count, not sends)))

    else:
        turned = embeddings.reshape(rows, count, chunks, part, width).transpose(1, 2, 3, 0, 4)
        me = lax.axis_index("emb")

        def cut(names):
            for m, c in names:
                sends[m, c] = lax.dynamic_index_in_dim(turned, target(me, m, count), 0, keepdims=False)[c]

    arrived = {}

    def forward(names):
        for m, c in names:
            arrived[m, c] = send(sends[m, c], m, "emb", count)

    cut([(m, 0) for m in far[:2]])
    forward([(m, 0) for m in far[:2]])
    cut([(m, 0) for m in far[2:] + near + [0]] + [(m, c) for c in range(1, chunks) for m in far + near + [0]])
    forward([(m, 0) for m in far[2:] + near + [0]])
    weights = []
    for q in range(others):
        weights.append(send(w_lcb, q, "dp", others))
    for c in range(1, chunks):
        forward([(m, c) for m in near + far + [0]])

    returned = {}
    for c in range(chunks):
        done = layer([arrived[m, c] for m in range(count)], weights, machine_projection.T, w_fmb)
        for m in near + far + [0]:
            returned[m, c] = send(done[m], m, "emb", count, back=True)

    if fast:
        out = None
        for messages in [[0] + near] + [[m] for m in sorted(far)]:
            pieces = [returned[m, c] for m in messages for c in range(chunks)]
            out = merge(out, pieces, ln_gain, ln_bias, messages, chunks, count, samples)
        return out
    me = lax.axis_index("emb")
    stacked = jnp.stack([jnp.concatenate([returned[m, c] for c in range(chunks)]) for m in range(count)])
    finished = (stacked.astype(jnp.float32) * ln_gain + ln_bias).astype(jnp.bfloat16)
    order = jnp.stack([_message_to(me, j, count) for j in range(count)])
    finished = jnp.take(finished, order, axis=0)
    return finished.transpose(2, 0, 1, 3).reshape(rows, samples, width)


def _message_to(me, j, count):
    if count & (count - 1) == 0:
        return me ^ j
    return lax.rem(j - me + count, count)


def solution(mesh):
    return jax.shard_map(
        body,
        mesh=mesh,
        in_specs=(P("emb", "dp", None), P(), P("dp", None), P(), P("emb", None), P("emb", None)),
        out_specs=P("emb", "dp", None),
        check_vma=False,
    )
```

```python
import functools

import jax
import jax.numpy as jnp
from jax import lax
from jax.experimental import pallas as pl
from jax.experimental.pallas import tpu as pltpu
from jax.sharding import PartitionSpec as P


GROUP = 8
EPS = 1e-05


def target(me, m, count):
    if count & (count - 1) == 0:
        return me ^ m
    return lax.rem(me + m, count)


def origin(me, m, count):
    if count & (count - 1) == 0:
        return me ^ m
    return lax.rem(me + count - m, count)


def sides(count):
    half = count // 2
    return sorted(range(half, count), key=lambda m: (-(m // 2), m)), list(range(1, half))


def chunk_count(share):
    return 2 if share % 2 == 0 else 1


def send(value, m, axis, count, back=False):
    if m == 0:
        return value
    pairs = []
    for i in range(count):
        j = i ^ m if count & (count - 1) == 0 else (i + m) % count
        pairs.append((j, i) if back else (i, j))
    return lax.ppermute(value, axis, pairs)


def row_block(rows):
    size = 32
    while rows % size:
        size //= 2
    return size


def pick_matrix(height, width, inner_out, inner_in):
    i = lax.broadcasted_iota(jnp.int32, (height, width), 0)
    j = lax.broadcasted_iota(jnp.int32, (height, width), 1)
    hit = (i // inner_out == j % inner_in) & (i % inner_out == j // inner_in)
    return jnp.where(hit, 1.0, 0.0).astype(jnp.bfloat16)


def split_kernel(messages, chunks, count, x_ref, *refs):
    outs = refs[: len(messages)]
    landed, sems = refs[len(messages) :]
    rows, _, width = x_ref.shape
    me = lax.axis_index("emb")
    distinct = sorted({m for m, _ in messages}, key=[m for m, _ in messages].index)

    def fetch(k):
        first = pl.multiple_of(target(me, distinct[k], count) * GROUP, GROUP)
        return pltpu.make_async_copy(x_ref.at[:, pl.ds(first, GROUP), :], landed.at[k], sems.at[k])

    for k in range(len(distinct)):
        fetch(k).start()
    block = row_block(rows)
    part = GROUP // chunks
    pick = pick_matrix(GROUP * block, block * GROUP, block, GROUP)
    for k, m in enumerate(distinct):
        fetch(k).wait()
        for q, (m2, c) in enumerate(messages):
            if m2 != m:
                continue
            for b in range(rows // block):
                piece = landed[k, b * block : (b + 1) * block].reshape(block * GROUP, width)
                moved = jnp.dot(
                    pick[c * part * block : (c + 1) * part * block], piece, preferred_element_type=jnp.float32
                )
                outs[q][:, b * block : (b + 1) * block, :] = moved.astype(jnp.bfloat16).reshape(part, block, width)


def lift_kernel(m, count, x_ref, out_ref, sem):
    first = pl.multiple_of(target(lax.axis_index("emb"), m, count) * GROUP, GROUP)
    copy = pltpu.make_async_copy(x_ref.at[:, pl.ds(first, GROUP), :], out_ref, sem)
    copy.start()
    copy.wait()


def lift(x, m, count):
    rows, _, width = x.shape
    return pl.pallas_call(
        functools.partial(lift_kernel, m, count),
        out_shape=jax.ShapeDtypeStruct((rows, GROUP, width), jnp.bfloat16),
        in_specs=[pl.BlockSpec(memory_space=pltpu.HBM)],
        out_specs=pl.BlockSpec(memory_space=pltpu.VMEM),
        scratch_shapes=[pltpu.SemaphoreType.DMA],
        compiler_params=pltpu.CompilerParams(vmem_limit_bytes=12 * 1024 * 1024),
        cost_estimate=pl.CostEstimate(flops=10**7, bytes_accessed=10**6, transcendentals=0),
        name="lift",
    )(pltpu.with_memory_space_constraint(x, pltpu.HBM))


def split(x, messages, chunks, count):
    rows, _, width = x.shape
    part = GROUP // chunks
    distinct = len({m for m, _ in messages})
    out = jax.ShapeDtypeStruct((part, rows, width), jnp.bfloat16)
    return pl.pallas_call(
        functools.partial(split_kernel, messages, chunks, count),
        out_shape=[out] * len(messages),
        in_specs=[pl.BlockSpec(memory_space=pltpu.HBM)],
        out_specs=[pl.BlockSpec(memory_space=pltpu.VMEM)] * len(messages),
        scratch_shapes=[
            pltpu.VMEM((distinct, rows, GROUP, width), jnp.bfloat16),
            pltpu.SemaphoreType.DMA((distinct,)),
        ],
        compiler_params=pltpu.CompilerParams(vmem_limit_bytes=12 * 1024 * 1024),
        cost_estimate=pl.CostEstimate(flops=10**8, bytes_accessed=10**6, transcendentals=0),
        name="split",
    )(x)


def merge_kernel(messages, chunks, count, first, *refs):
    pieces = refs[: len(messages) * chunks]
    gain_ref, bias_ref = refs[len(messages) * chunks : len(messages) * chunks + 2]
    rest = refs[len(messages) * chunks + 2 :]
    out_ref, ready, sems = rest if first else rest[1:]
    _, rows, width = pieces[0].shape
    me = lax.axis_index("emb")
    block = row_block(rows)
    pick = pick_matrix(block * GROUP, GROUP * block, GROUP, block)
    blocks = rows // block
    copies = []
    for k, m in enumerate(messages):
        start = pl.multiple_of(target(me, m, count) * GROUP, GROUP)
        for b in range(blocks):
            here = slice(b * block, (b + 1) * block)
            gain, bias = gain_ref[here], bias_ref[here]
            done = [
                (pieces[k * chunks + c][:, here, :].astype(jnp.float32) * gain[None] + bias[None]).astype(jnp.bfloat16)
                for c in range(chunks)
            ]
            done = jnp.concatenate(done, axis=0).reshape(GROUP * block, width)
            moved = jnp.dot(pick, done, preferred_element_type=jnp.float32)
            ready[k, here] = moved.astype(jnp.bfloat16).reshape(block, GROUP, width)
            copies.append(
                pltpu.make_async_copy(
                    ready.at[k, here], out_ref.at[here, pl.ds(start, GROUP), :], sems.at[k * blocks + b]
                )
            )
            copies[-1].start()
    for copy in copies:
        copy.wait()


def merge(out, pieces, gain, bias, messages, chunks, count, samples):
    _, rows, width = pieces[0].shape
    first = out is None
    vmem = pl.BlockSpec(memory_space=pltpu.VMEM)
    hbm = pl.BlockSpec(memory_space=pl.ANY)
    operands = list(pieces) + [gain, bias] + ([] if first else [out])
    return pl.pallas_call(
        functools.partial(merge_kernel, messages, chunks, count, first),
        out_shape=jax.ShapeDtypeStruct((rows, samples, width), jnp.bfloat16),
        in_specs=[vmem] * (len(pieces) + 2) + ([] if first else [hbm]),
        out_specs=hbm,
        input_output_aliases={} if first else {len(operands) - 1: 0},
        scratch_shapes=[
            pltpu.VMEM((len(messages), rows, GROUP, width), jnp.bfloat16),
            pltpu.SemaphoreType.DMA((len(messages) * (rows // row_block(rows)),)),
        ],
        compiler_params=pltpu.CompilerParams(vmem_limit_bytes=12 * 1024 * 1024),
        cost_estimate=pl.CostEstimate(flops=10**8, bytes_accessed=10**6, transcendentals=0),
        name="merge",
    )(*operands)


def layer_kernel(count, pieces_w, raw, chunk, *refs):
    blocks = list(refs[:count])
    weights = refs[count : count + pieces_w]
    proj_ref, fmb_ref = refs[count + pieces_w : count + pieces_w + 2]
    outs = refs[count + pieces_w + 2 : count + pieces_w + 2 + count]
    full_w, held, mixed = refs[count + pieces_w + 2 + count :][:3]
    part, rows, width = blocks[0].shape
    if raw is not None:
        turned = refs[-1]
        block = row_block(rows)
        pick = pick_matrix(GROUP * block, block * GROUP, block, GROUP)[chunk * part * block : (chunk + 1) * part * block]
        for b in range(rows // block):
            piece = blocks[raw][b * block : (b + 1) * block].reshape(block * GROUP, width)
            moved = jnp.dot(pick, piece, preferred_element_type=jnp.float32)
            turned[:, b * block : (b + 1) * block, :] = moved.astype(jnp.bfloat16).reshape(part, block, width)
        blocks[raw] = turned
    total = count * rows
    me = lax.axis_index("emb")
    mine = lax.axis_index("dp")
    share_w = weights[0].shape[0]
    for q in range(pieces_w):
        full_w[pl.ds(pl.multiple_of(origin(mine, q, pieces_w) * share_w, share_w), share_w), :] = weights[q][...]
    entries = float(total * width)
    starts = [pl.multiple_of(origin(me, m, count) * rows, rows) for m in range(count)]

    def one(s, _):
        for m in range(count):
            held[pl.ds(starts[m], rows), :] = blocks[m][s]
        x = held[...]
        summed = jnp.dot(proj_ref[...], x, preferred_element_type=jnp.float32)
        factor = summed.astype(jnp.bfloat16)
        inner = lax.dot_general(x, factor, (((1,), (1,)), ((), ())), preferred_element_type=jnp.float32)
        fmb = jnp.dot(inner.astype(jnp.bfloat16), fmb_ref[...], preferred_element_type=jnp.float32)
        compressed = jnp.dot(full_w[...], x, preferred_element_type=jnp.float32)
        value = x.astype(jnp.float32) + compressed + fmb
        mixed[...] = value
        average = jnp.sum(value) / entries
        centered = mixed[...] - average
        spread = jnp.sum(centered * centered) / entries
        scale = lax.rsqrt(jnp.full((1, width), spread + EPS, jnp.float32))
        for m in range(count):
            outs[m][s] = ((mixed[pl.ds(starts[m], rows), :] - average) * scale).astype(jnp.bfloat16)
        return 0

    lax.fori_loop(0, part, one, 0)


def layer(blocks, weights, proj, w_fmb, raw, chunk):
    part, rows, width = blocks[0].shape
    count = len(blocks)
    total = count * rows
    vmem = pl.BlockSpec(memory_space=pltpu.VMEM)
    return pl.pallas_call(
        functools.partial(layer_kernel, count, len(weights), raw, chunk),
        out_shape=[jax.ShapeDtypeStruct((part, rows, width), jnp.bfloat16)] * count,
        in_specs=[vmem] * (count + len(weights) + 2),
        out_specs=[vmem] * count,
        scratch_shapes=[
            pltpu.VMEM((weights[0].shape[0] * len(weights), total), jnp.bfloat16),
            pltpu.VMEM((total, width), jnp.bfloat16),
            pltpu.VMEM((total, width), jnp.float32),
        ]
        + ([] if raw is None else [pltpu.VMEM((part, rows, width), jnp.bfloat16)]),
        compiler_params=pltpu.CompilerParams(vmem_limit_bytes=12 * 1024 * 1024),
        cost_estimate=pl.CostEstimate(
            flops=2 * part * total * total * width, bytes_accessed=4 * part * total * width, transcendentals=0
        ),
        name="layer",
    )(*blocks, *weights, proj, w_fmb)


def body(embeddings, machine_projection, w_lcb, w_fmb, ln_gain, ln_bias):
    rows, samples, width = embeddings.shape
    count = lax.axis_size("emb")
    others = lax.axis_size("dp")
    share = samples // count
    chunks = chunk_count(share)
    part = share // chunks
    far, near = sides(count)
    fast = share == GROUP
    sends = {}

    if fast:

        def cut(names):
            sends.update(zip(names, split(embeddings, names, chunks, count)))

    else:
        turned = embeddings.reshape(rows, count, chunks, part, width).transpose(1, 2, 3, 0, 4)
        me = lax.axis_index("emb")

        def cut(names):
            for m, c in names:
                sends[m, c] = lax.dynamic_index_in_dim(turned, target(me, m, count), 0, keepdims=False)[c]

    arrived = {}

    def forward(names):
        for m, c in names:
            arrived[m, c] = send(sends[m, c], m, "emb", count)

    raw = far[0] if fast else None
    if fast:
        lifted = lift(embeddings, raw, count)
        lifted = send(lifted, raw, "emb", count)
        arrived.update({(raw, c): lifted for c in range(chunks)})
    cut([(m, c) for c in range(chunks) for m in far + near + [0] if m != raw])
    forward([(m, 0) for m in far + near + [0] if m != raw])
    weights = []
    for q in range(others):
        weights.append(send(w_lcb, q, "dp", others))
    for c in range(1, chunks):
        forward([(m, c) for m in near + far + [0] if m != raw])

    returned = {}
    for c in range(chunks):
        done = layer([arrived[m, c] for m in range(count)], weights, machine_projection.T, w_fmb, raw, c)
        for m in near + far + [0]:
            returned[m, c] = send(done[m], m, "emb", count, back=True)

    if fast:
        out = None
        for messages in [[0] + near] + [[m] for m in sorted(far)]:
            pieces = [returned[m, c] for m in messages for c in range(chunks)]
            out = merge(out, pieces, ln_gain, ln_bias, messages, chunks, count, samples)
        return out
    me = lax.axis_index("emb")
    stacked = jnp.stack([jnp.concatenate([returned[m, c] for c in range(chunks)]) for m in range(count)])
    finished = (stacked.astype(jnp.float32) * ln_gain + ln_bias).astype(jnp.bfloat16)
    order = jnp.stack([_message_to(me, j, count) for j in range(count)])
    finished = jnp.take(finished, order, axis=0)
    return finished.transpose(2, 0, 1, 3).reshape(rows, samples, width)


def _message_to(me, j, count):
    if count & (count - 1) == 0:
        return me ^ j
    return lax.rem(j - me + count, count)


def solution(mesh):
    return jax.shard_map(
        body,
        mesh=mesh,
        in_specs=(P("emb", "dp", None), P(), P("dp", None), P(), P("emb", None), P("emb", None)),
        out_specs=P("emb", "dp", None),
        check_vma=False,
    )
```

```python
import functools

import jax
import jax.numpy as jnp
from jax import lax
from jax.experimental import pallas as pl
from jax.experimental.pallas import tpu as pltpu
from jax.sharding import PartitionSpec as P


GROUP = 8
EPS = 1e-05


def target(me, m, count):
    if count & (count - 1) == 0:
        return me ^ m
    return lax.rem(me + m, count)


def origin(me, m, count):
    if count & (count - 1) == 0:
        return me ^ m
    return lax.rem(me + count - m, count)


def sides(count):
    half = count // 2
    return sorted(range(half, count), key=lambda m: (-(m // 2), m)), list(range(1, half))


def chunk_count(share):
    return 2 if share % 2 == 0 else 1


def send(value, m, axis, count, back=False):
    if m == 0:
        return value
    pairs = []
    for i in range(count):
        j = i ^ m if count & (count - 1) == 0 else (i + m) % count
        pairs.append((j, i) if back else (i, j))
    return lax.ppermute(value, axis, pairs)


def row_block(rows):
    size = 32
    while rows % size:
        size //= 2
    return size


def pick_matrix(height, width, inner_out, inner_in):
    i = lax.broadcasted_iota(jnp.int32, (height, width), 0)
    j = lax.broadcasted_iota(jnp.int32, (height, width), 1)
    hit = (i // inner_out == j % inner_in) & (i % inner_out == j // inner_in)
    return jnp.where(hit, 1.0, 0.0).astype(jnp.bfloat16)


def split_kernel(messages, chunks, count, x_ref, *refs):
    outs = refs[: len(messages)]
    back_ref, landed, sems = refs[len(messages) :]
    rows, _, width = x_ref.shape
    me = lax.axis_index("emb")
    distinct = sorted({m for m, _ in messages}, key=[m for m, _ in messages].index)

    def fetch(k):
        first = pl.multiple_of(target(me, distinct[k], count) * GROUP, GROUP)
        return pltpu.make_async_copy(x_ref.at[:, pl.ds(first, GROUP), :], landed.at[k], sems.at[k])

    for k in range(len(distinct)):
        fetch(k).start()
    block = row_block(rows)
    part = GROUP // chunks
    pick = pick_matrix(GROUP * block, block * GROUP, block, GROUP)
    back_ref[...] = pick_matrix(block * GROUP, GROUP * block, GROUP, block)
    for k, m in enumerate(distinct):
        fetch(k).wait()
        for q, (m2, c) in enumerate(messages):
            if m2 != m:
                continue
            for b in range(rows // block):
                piece = landed[k, b * block : (b + 1) * block].reshape(block * GROUP, width)
                moved = jnp.dot(
                    pick[c * part * block : (c + 1) * part * block], piece, preferred_element_type=jnp.float32
                )
                outs[q][:, b * block : (b + 1) * block, :] = moved.astype(jnp.bfloat16).reshape(part, block, width)


def lift_kernel(m, count, x_ref, out_ref, sem):
    first = pl.multiple_of(target(lax.axis_index("emb"), m, count) * GROUP, GROUP)
    copy = pltpu.make_async_copy(x_ref.at[:, pl.ds(first, GROUP), :], out_ref, sem)
    copy.start()
    copy.wait()


def lift(x, m, count):
    rows, _, width = x.shape
    return pl.pallas_call(
        functools.partial(lift_kernel, m, count),
        out_shape=jax.ShapeDtypeStruct((rows, GROUP, width), jnp.bfloat16),
        in_specs=[pl.BlockSpec(memory_space=pltpu.HBM)],
        out_specs=pl.BlockSpec(memory_space=pltpu.VMEM),
        scratch_shapes=[pltpu.SemaphoreType.DMA],
        compiler_params=pltpu.CompilerParams(vmem_limit_bytes=12 * 1024 * 1024),
        cost_estimate=pl.CostEstimate(flops=10**7, bytes_accessed=10**6, transcendentals=0),
        name="lift",
    )(pltpu.with_memory_space_constraint(x, pltpu.HBM))


def split(x, messages, chunks, count):
    rows, _, width = x.shape
    part = GROUP // chunks
    distinct = len({m for m, _ in messages})
    out = jax.ShapeDtypeStruct((part, rows, width), jnp.bfloat16)
    return pl.pallas_call(
        functools.partial(split_kernel, messages, chunks, count),
        out_shape=[out] * len(messages) + [jax.ShapeDtypeStruct((row_block(rows) * GROUP,) * 2, jnp.bfloat16)],
        in_specs=[pl.BlockSpec(memory_space=pltpu.HBM)],
        out_specs=[pl.BlockSpec(memory_space=pltpu.VMEM)] * (len(messages) + 1),
        scratch_shapes=[
            pltpu.VMEM((distinct, rows, GROUP, width), jnp.bfloat16),
            pltpu.SemaphoreType.DMA((distinct,)),
        ],
        compiler_params=pltpu.CompilerParams(vmem_limit_bytes=12 * 1024 * 1024),
        cost_estimate=pl.CostEstimate(flops=10**8, bytes_accessed=10**6, transcendentals=0),
        name="split",
    )(x)


def merge_kernel(messages, chunks, count, first, *refs):
    pieces = refs[: len(messages) * chunks]
    gain_ref, bias_ref, pick_ref = refs[len(messages) * chunks : len(messages) * chunks + 3]
    rest = refs[len(messages) * chunks + 3 :]
    out_ref, ready, sems = rest if first else rest[1:]
    _, rows, width = pieces[0].shape
    me = lax.axis_index("emb")
    block = row_block(rows)
    pick = pick_ref[...]
    blocks = rows // block
    copies = []
    for k, m in enumerate(messages):
        start = pl.multiple_of(target(me, m, count) * GROUP, GROUP)
        for b in range(blocks):
            here = slice(b * block, (b + 1) * block)
            gain, bias = gain_ref[here], bias_ref[here]
            done = [
                (pieces[k * chunks + c][:, here, :].astype(jnp.float32) * gain[None] + bias[None]).astype(jnp.bfloat16)
                for c in range(chunks)
            ]
            done = jnp.concatenate(done, axis=0).reshape(GROUP * block, width)
            moved = jnp.dot(pick, done, preferred_element_type=jnp.float32)
            ready[k, here] = moved.astype(jnp.bfloat16).reshape(block, GROUP, width)
            copies.append(
                pltpu.make_async_copy(
                    ready.at[k, here], out_ref.at[here, pl.ds(start, GROUP), :], sems.at[k * blocks + b]
                )
            )
            copies[-1].start()
    for copy in copies:
        copy.wait()


def merge(out, pieces, gain, bias, pick, messages, chunks, count, samples):
    _, rows, width = pieces[0].shape
    first = out is None
    vmem = pl.BlockSpec(memory_space=pltpu.VMEM)
    hbm = pl.BlockSpec(memory_space=pl.ANY)
    operands = list(pieces) + [gain, bias, pick] + ([] if first else [out])
    return pl.pallas_call(
        functools.partial(merge_kernel, messages, chunks, count, first),
        out_shape=jax.ShapeDtypeStruct((rows, samples, width), jnp.bfloat16),
        in_specs=[vmem] * (len(pieces) + 3) + ([] if first else [hbm]),
        out_specs=hbm,
        input_output_aliases={} if first else {len(operands) - 1: 0},
        scratch_shapes=[
            pltpu.VMEM((len(messages), rows, GROUP, width), jnp.bfloat16),
            pltpu.SemaphoreType.DMA((len(messages) * (rows // row_block(rows)),)),
        ],
        compiler_params=pltpu.CompilerParams(vmem_limit_bytes=12 * 1024 * 1024),
        cost_estimate=pl.CostEstimate(flops=10**8, bytes_accessed=10**6, transcendentals=0),
        name="merge",
    )(*operands)


def layer_kernel(count, pieces_w, raw, chunk, *refs):
    blocks = list(refs[:count])
    weights = refs[count : count + pieces_w]
    proj_ref, fmb_ref = refs[count + pieces_w : count + pieces_w + 2]
    outs = refs[count + pieces_w + 2 : count + pieces_w + 2 + count]
    full_w, held, mixed = refs[count + pieces_w + 2 + count :][:3]
    part, rows, width = blocks[0].shape
    if raw is not None:
        turned = refs[-1]
        block = row_block(rows)
        pick = pick_matrix(GROUP * block, block * GROUP, block, GROUP)[chunk * part * block : (chunk + 1) * part * block]
        for b in range(rows // block):
            piece = blocks[raw][b * block : (b + 1) * block].reshape(block * GROUP, width)
            moved = jnp.dot(pick, piece, preferred_element_type=jnp.float32)
            turned[:, b * block : (b + 1) * block, :] = moved.astype(jnp.bfloat16).reshape(part, block, width)
        blocks[raw] = turned
    total = count * rows
    me = lax.axis_index("emb")
    mine = lax.axis_index("dp")
    share_w = weights[0].shape[0]
    for q in range(pieces_w):
        full_w[pl.ds(pl.multiple_of(origin(mine, q, pieces_w) * share_w, share_w), share_w), :] = weights[q][...]
    entries = float(total * width)
    starts = [pl.multiple_of(origin(me, m, count) * rows, rows) for m in range(count)]

    def one(s, _):
        for m in range(count):
            held[pl.ds(starts[m], rows), :] = blocks[m][s]
        x = held[...]
        summed = jnp.dot(proj_ref[...], x, preferred_element_type=jnp.float32)
        factor = summed.astype(jnp.bfloat16)
        inner = lax.dot_general(x, factor, (((1,), (1,)), ((), ())), preferred_element_type=jnp.float32)
        fmb = jnp.dot(inner.astype(jnp.bfloat16), fmb_ref[...], preferred_element_type=jnp.float32)
        compressed = jnp.dot(full_w[...], x, preferred_element_type=jnp.float32)
        value = x.astype(jnp.float32) + compressed + fmb
        mixed[...] = value
        average = jnp.sum(value) / entries
        centered = mixed[...] - average
        spread = jnp.sum(centered * centered) / entries
        scale = lax.rsqrt(jnp.full((1, width), spread + EPS, jnp.float32))
        for m in range(count):
            outs[m][s] = ((mixed[pl.ds(starts[m], rows), :] - average) * scale).astype(jnp.bfloat16)
        return 0

    lax.fori_loop(0, part, one, 0)


def layer(blocks, weights, proj, w_fmb, raw, chunk):
    part, rows, width = blocks[0].shape
    count = len(blocks)
    total = count * rows
    vmem = pl.BlockSpec(memory_space=pltpu.VMEM)
    return pl.pallas_call(
        functools.partial(layer_kernel, count, len(weights), raw, chunk),
        out_shape=[jax.ShapeDtypeStruct((part, rows, width), jnp.bfloat16)] * count,
        in_specs=[vmem] * (count + len(weights) + 2),
        out_specs=[vmem] * count,
        scratch_shapes=[
            pltpu.VMEM((weights[0].shape[0] * len(weights), total), jnp.bfloat16),
            pltpu.VMEM((total, width), jnp.bfloat16),
            pltpu.VMEM((total, width), jnp.float32),
        ]
        + ([] if raw is None else [pltpu.VMEM((part, rows, width), jnp.bfloat16)]),
        compiler_params=pltpu.CompilerParams(vmem_limit_bytes=12 * 1024 * 1024),
        cost_estimate=pl.CostEstimate(
            flops=2 * part * total * total * width, bytes_accessed=4 * part * total * width, transcendentals=0
        ),
        name="layer",
    )(*blocks, *weights, proj, w_fmb)


def body(embeddings, machine_projection, w_lcb, w_fmb, ln_gain, ln_bias):
    rows, samples, width = embeddings.shape
    count = lax.axis_size("emb")
    others = lax.axis_size("dp")
    share = samples // count
    chunks = chunk_count(share)
    part = share // chunks
    far, near = sides(count)
    fast = share == GROUP
    sends = {}

    if fast:

        def cut(names):
            *cuts, sends["pick"] = split(embeddings, names, chunks, count)
            sends.update(zip(names, cuts))

    else:
        turned = embeddings.reshape(rows, count, chunks, part, width).transpose(1, 2, 3, 0, 4)
        me = lax.axis_index("emb")

        def cut(names):
            for m, c in names:
                sends[m, c] = lax.dynamic_index_in_dim(turned, target(me, m, count), 0, keepdims=False)[c]

    arrived = {}

    def forward(names):
        for m, c in names:
            arrived[m, c] = send(sends[m, c], m, "emb", count)

    raw = far[0] if fast else None
    if fast:
        lifted = lift(embeddings, raw, count)
        lifted = send(lifted, raw, "emb", count)
        arrived.update({(raw, c): lifted for c in range(chunks)})
    cut([(m, c) for c in range(chunks) for m in far + near + [0] if m != raw])
    forward([(m, 0) for m in far + near + [0] if m != raw])
    weights = []
    for q in range(others):
        weights.append(send(w_lcb, q, "dp", others))
    for c in range(1, chunks):
        forward([(m, c) for m in near + far + [0] if m != raw])

    returned = {}
    for c in range(chunks):
        done = layer([arrived[m, c] for m in range(count)], weights, machine_projection.T, w_fmb, raw, c)
        for m in near + far + [0]:
            returned[m, c] = send(done[m], m, "emb", count, back=True)

    if fast:
        out = None
        for messages in [[0] + near] + [[m] for m in sorted(far)]:
            pieces = [returned[m, c] for m in messages for c in range(chunks)]
            out = merge(out, pieces, ln_gain, ln_bias, sends["pick"], messages, chunks, count, samples)
        return out
    me = lax.axis_index("emb")
    stacked = jnp.stack([jnp.concatenate([returned[m, c] for c in range(chunks)]) for m in range(count)])
    finished = (stacked.astype(jnp.float32) * ln_gain + ln_bias).astype(jnp.bfloat16)
    order = jnp.stack([_message_to(me, j, count) for j in range(count)])
    finished = jnp.take(finished, order, axis=0)
    return finished.transpose(2, 0, 1, 3).reshape(rows, samples, width)


def _message_to(me, j, count):
    if count & (count - 1) == 0:
        return me ^ j
    return lax.rem(j - me + count, count)


def solution(mesh):
    return jax.shard_map(
        body,
        mesh=mesh,
        in_specs=(P("emb", "dp", None), P(), P("dp", None), P(), P("emb", None), P("emb", None)),
        out_specs=P("emb", "dp", None),
        check_vma=False,
    )
```

```python
import functools

import jax
import jax.numpy as jnp
from jax import lax
from jax.experimental import pallas as pl
from jax.experimental.pallas import tpu as pltpu
from jax.sharding import PartitionSpec as P


GROUP = 8
EPS = 1e-05


def target(me, m, count):
    if count & (count - 1) == 0:
        return me ^ m
    return lax.rem(me + m, count)


def origin(me, m, count):
    if count & (count - 1) == 0:
        return me ^ m
    return lax.rem(me + count - m, count)


def sides(count):
    half = count // 2
    return sorted(range(half, count), key=lambda m: (-(m // 2), m)), list(range(1, half))


def chunk_count(share):
    return 2 if share % 2 == 0 else 1


def send(value, m, axis, count, back=False):
    if m == 0:
        return value
    pairs = []
    for i in range(count):
        j = i ^ m if count & (count - 1) == 0 else (i + m) % count
        pairs.append((j, i) if back else (i, j))
    return lax.ppermute(value, axis, pairs)


def row_block(rows):
    size = 32
    while rows % size:
        size //= 2
    return size


def merge_block(rows):
    return min(row_block(rows), 16)


def pick_matrix(height, width, inner_out, inner_in):
    i = lax.broadcasted_iota(jnp.int32, (height, width), 0)
    j = lax.broadcasted_iota(jnp.int32, (height, width), 1)
    hit = (i // inner_out == j % inner_in) & (i % inner_out == j // inner_in)
    return jnp.where(hit, 1.0, 0.0).astype(jnp.bfloat16)


def split_kernel(messages, chunks, count, x_ref, *refs):
    outs = refs[: len(messages)]
    back_ref, landed, sems = refs[len(messages) :]
    rows, _, width = x_ref.shape
    me = lax.axis_index("emb")
    distinct = sorted({m for m, _ in messages}, key=[m for m, _ in messages].index)

    def fetch(k):
        first = pl.multiple_of(target(me, distinct[k], count) * GROUP, GROUP)
        return pltpu.make_async_copy(x_ref.at[:, pl.ds(first, GROUP), :], landed.at[k], sems.at[k])

    for k in range(len(distinct)):
        fetch(k).start()
    block = row_block(rows)
    part = GROUP // chunks
    pick = pick_matrix(GROUP * block, block * GROUP, block, GROUP)
    turn = merge_block(rows)
    back_ref[...] = pick_matrix(turn * GROUP, GROUP * turn, GROUP, turn)
    for k, m in enumerate(distinct):
        fetch(k).wait()
        for q, (m2, c) in enumerate(messages):
            if m2 != m:
                continue
            for b in range(rows // block):
                piece = landed[k, b * block : (b + 1) * block].reshape(block * GROUP, width)
                moved = jnp.dot(
                    pick[c * part * block : (c + 1) * part * block], piece, preferred_element_type=jnp.float32
                )
                outs[q][:, b * block : (b + 1) * block, :] = moved.astype(jnp.bfloat16).reshape(part, block, width)


def lift_kernel(m, count, x_ref, out_ref, sem):
    first = pl.multiple_of(target(lax.axis_index("emb"), m, count) * GROUP, GROUP)
    copy = pltpu.make_async_copy(x_ref.at[:, pl.ds(first, GROUP), :], out_ref, sem)
    copy.start()
    copy.wait()


def lift(x, m, count):
    rows, _, width = x.shape
    return pl.pallas_call(
        functools.partial(lift_kernel, m, count),
        out_shape=jax.ShapeDtypeStruct((rows, GROUP, width), jnp.bfloat16),
        in_specs=[pl.BlockSpec(memory_space=pltpu.HBM)],
        out_specs=pl.BlockSpec(memory_space=pltpu.VMEM),
        scratch_shapes=[pltpu.SemaphoreType.DMA],
        compiler_params=pltpu.CompilerParams(vmem_limit_bytes=12 * 1024 * 1024),
        cost_estimate=pl.CostEstimate(flops=10**7, bytes_accessed=10**6, transcendentals=0),
        name="lift",
    )(pltpu.with_memory_space_constraint(x, pltpu.HBM))


def split(x, messages, chunks, count):
    rows, _, width = x.shape
    part = GROUP // chunks
    distinct = len({m for m, _ in messages})
    out = jax.ShapeDtypeStruct((part, rows, width), jnp.bfloat16)
    return pl.pallas_call(
        functools.partial(split_kernel, messages, chunks, count),
        out_shape=[out] * len(messages) + [jax.ShapeDtypeStruct((merge_block(rows) * GROUP,) * 2, jnp.bfloat16)],
        in_specs=[pl.BlockSpec(memory_space=pltpu.HBM)],
        out_specs=[pl.BlockSpec(memory_space=pltpu.VMEM)] * (len(messages) + 1),
        scratch_shapes=[
            pltpu.VMEM((distinct, rows, GROUP, width), jnp.bfloat16),
            pltpu.SemaphoreType.DMA((distinct,)),
        ],
        compiler_params=pltpu.CompilerParams(vmem_limit_bytes=12 * 1024 * 1024),
        cost_estimate=pl.CostEstimate(flops=10**8, bytes_accessed=10**6, transcendentals=0),
        name="split",
    )(x)


def merge_kernel(messages, chunks, count, first, *refs):
    pieces = refs[: len(messages) * chunks]
    gain_ref, bias_ref, pick_ref = refs[len(messages) * chunks : len(messages) * chunks + 3]
    rest = refs[len(messages) * chunks + 3 :]
    out_ref, ready, sems = rest if first else rest[1:]
    _, rows, width = pieces[0].shape
    me = lax.axis_index("emb")
    block = merge_block(rows)
    pick = pick_ref[...]
    blocks = rows // block
    copies = []
    for k, m in enumerate(messages):
        start = pl.multiple_of(target(me, m, count) * GROUP, GROUP)
        for b in range(blocks):
            here = slice(b * block, (b + 1) * block)
            gain, bias = gain_ref[here], bias_ref[here]
            done = [
                (pieces[k * chunks + c][:, here, :].astype(jnp.float32) * gain[None] + bias[None]).astype(jnp.bfloat16)
                for c in range(chunks)
            ]
            done = jnp.concatenate(done, axis=0).reshape(GROUP * block, width)
            moved = jnp.dot(pick, done, preferred_element_type=jnp.float32)
            ready[k, here] = moved.astype(jnp.bfloat16).reshape(block, GROUP, width)
            copies.append(
                pltpu.make_async_copy(
                    ready.at[k, here], out_ref.at[here, pl.ds(start, GROUP), :], sems.at[k * blocks + b]
                )
            )
            copies[-1].start()
    for copy in copies:
        copy.wait()


def merge(out, pieces, gain, bias, pick, messages, chunks, count, samples):
    _, rows, width = pieces[0].shape
    first = out is None
    vmem = pl.BlockSpec(memory_space=pltpu.VMEM)
    hbm = pl.BlockSpec(memory_space=pl.ANY)
    operands = list(pieces) + [gain, bias, pick] + ([] if first else [out])
    return pl.pallas_call(
        functools.partial(merge_kernel, messages, chunks, count, first),
        out_shape=jax.ShapeDtypeStruct((rows, samples, width), jnp.bfloat16),
        in_specs=[vmem] * (len(pieces) + 3) + ([] if first else [hbm]),
        out_specs=hbm,
        input_output_aliases={} if first else {len(operands) - 1: 0},
        scratch_shapes=[
            pltpu.VMEM((len(messages), rows, GROUP, width), jnp.bfloat16),
            pltpu.SemaphoreType.DMA((len(messages) * (rows // merge_block(rows)),)),
        ],
        compiler_params=pltpu.CompilerParams(vmem_limit_bytes=12 * 1024 * 1024),
        cost_estimate=pl.CostEstimate(flops=10**8, bytes_accessed=10**6, transcendentals=0),
        name="merge",
    )(*operands)


def layer_kernel(count, pieces_w, raw, chunk, *refs):
    blocks = list(refs[:count])
    weights = refs[count : count + pieces_w]
    proj_ref, fmb_ref = refs[count + pieces_w : count + pieces_w + 2]
    outs = refs[count + pieces_w + 2 : count + pieces_w + 2 + count]
    full_w, held, mixed = refs[count + pieces_w + 2 + count :][:3]
    part, rows, width = blocks[0].shape
    if raw is not None:
        turned = refs[-1]
        block = row_block(rows)
        pick = pick_matrix(GROUP * block, block * GROUP, block, GROUP)[chunk * part * block : (chunk + 1) * part * block]
        for b in range(rows // block):
            piece = blocks[raw][b * block : (b + 1) * block].reshape(block * GROUP, width)
            moved = jnp.dot(pick, piece, preferred_element_type=jnp.float32)
            turned[:, b * block : (b + 1) * block, :] = moved.astype(jnp.bfloat16).reshape(part, block, width)
        blocks[raw] = turned
    total = count * rows
    me = lax.axis_index("emb")
    mine = lax.axis_index("dp")
    share_w = weights[0].shape[0]
    for q in range(pieces_w):
        full_w[pl.ds(pl.multiple_of(origin(mine, q, pieces_w) * share_w, share_w), share_w), :] = weights[q][...]
    entries = float(total * width)
    starts = [pl.multiple_of(origin(me, m, count) * rows, rows) for m in range(count)]

    def one(s, _):
        for m in range(count):
            held[pl.ds(starts[m], rows), :] = blocks[m][s]
        x = held[...]
        summed = jnp.dot(proj_ref[...], x, preferred_element_type=jnp.float32)
        factor = summed.astype(jnp.bfloat16)
        inner = lax.dot_general(x, factor, (((1,), (1,)), ((), ())), preferred_element_type=jnp.float32)
        fmb = jnp.dot(inner.astype(jnp.bfloat16), fmb_ref[...], preferred_element_type=jnp.float32)
        compressed = jnp.dot(full_w[...], x, preferred_element_type=jnp.float32)
        value = x.astype(jnp.float32) + compressed + fmb
        mixed[...] = value
        average = jnp.sum(value) / entries
        centered = mixed[...] - average
        spread = jnp.sum(centered * centered) / entries
        scale = lax.rsqrt(jnp.full((1, width), spread + EPS, jnp.float32))
        for m in range(count):
            outs[m][s] = ((mixed[pl.ds(starts[m], rows), :] - average) * scale).astype(jnp.bfloat16)
        return 0

    lax.fori_loop(0, part, one, 0)


def layer(blocks, weights, proj, w_fmb, raw, chunk):
    part, rows, width = blocks[0].shape
    count = len(blocks)
    total = count * rows
    vmem = pl.BlockSpec(memory_space=pltpu.VMEM)
    return pl.pallas_call(
        functools.partial(layer_kernel, count, len(weights), raw, chunk),
        out_shape=[jax.ShapeDtypeStruct((part, rows, width), jnp.bfloat16)] * count,
        in_specs=[vmem] * (count + len(weights) + 2),
        out_specs=[vmem] * count,
        scratch_shapes=[
            pltpu.VMEM((weights[0].shape[0] * len(weights), total), jnp.bfloat16),
            pltpu.VMEM((total, width), jnp.bfloat16),
            pltpu.VMEM((total, width), jnp.float32),
        ]
        + ([] if raw is None else [pltpu.VMEM((part, rows, width), jnp.bfloat16)]),
        compiler_params=pltpu.CompilerParams(vmem_limit_bytes=12 * 1024 * 1024),
        cost_estimate=pl.CostEstimate(
            flops=2 * part * total * total * width, bytes_accessed=4 * part * total * width, transcendentals=0
        ),
        name="layer",
    )(*blocks, *weights, proj, w_fmb)


def body(embeddings, machine_projection, w_lcb, w_fmb, ln_gain, ln_bias):
    rows, samples, width = embeddings.shape
    count = lax.axis_size("emb")
    others = lax.axis_size("dp")
    share = samples // count
    chunks = chunk_count(share)
    part = share // chunks
    far, near = sides(count)
    fast = share == GROUP
    sends = {}

    if fast:

        def cut(names):
            *cuts, sends["pick"] = split(embeddings, names, chunks, count)
            sends.update(zip(names, cuts))

    else:
        turned = embeddings.reshape(rows, count, chunks, part, width).transpose(1, 2, 3, 0, 4)
        me = lax.axis_index("emb")

        def cut(names):
            for m, c in names:
                sends[m, c] = lax.dynamic_index_in_dim(turned, target(me, m, count), 0, keepdims=False)[c]

    arrived = {}

    def forward(names):
        for m, c in names:
            arrived[m, c] = send(sends[m, c], m, "emb", count)

    raw = far[0] if fast else None
    if fast:
        lifted = lift(embeddings, raw, count)
        lifted = send(lifted, raw, "emb", count)
        arrived.update({(raw, c): lifted for c in range(chunks)})
    cut([(m, c) for c in range(chunks) for m in far + near + [0] if m != raw])
    forward([(m, 0) for m in far + near + [0] if m != raw])
    weights = []
    for q in range(others):
        weights.append(send(w_lcb, q, "dp", others))
    for c in range(1, chunks):
        forward([(m, c) for m in near + far + [0] if m != raw])

    returned = {}
    for c in range(chunks):
        done = layer([arrived[m, c] for m in range(count)], weights, machine_projection.T, w_fmb, raw, c)
        for m in near + far + [0]:
            returned[m, c] = send(done[m], m, "emb", count, back=True)

    if fast:
        out = None
        for messages in [[0] + near] + [[m] for m in sorted(far)]:
            pieces = [returned[m, c] for m in messages for c in range(chunks)]
            out = merge(out, pieces, ln_gain, ln_bias, sends["pick"], messages, chunks, count, samples)
        return out
    me = lax.axis_index("emb")
    stacked = jnp.stack([jnp.concatenate([returned[m, c] for c in range(chunks)]) for m in range(count)])
    finished = (stacked.astype(jnp.float32) * ln_gain + ln_bias).astype(jnp.bfloat16)
    order = jnp.stack([_message_to(me, j, count) for j in range(count)])
    finished = jnp.take(finished, order, axis=0)
    return finished.transpose(2, 0, 1, 3).reshape(rows, samples, width)


def _message_to(me, j, count):
    if count & (count - 1) == 0:
        return me ^ j
    return lax.rem(j - me + count, count)


def solution(mesh):
    return jax.shard_map(
        body,
        mesh=mesh,
        in_specs=(P("emb", "dp", None), P(), P("dp", None), P(), P("emb", None), P("emb", None)),
        out_specs=P("emb", "dp", None),
        check_vma=False,
    )
```
